8 devices in a mesh: dp: 1 (over z), vblk: 2 (over y), vocab: 4 (over x, core).
Axes of the slice: x: 2, y: 2, z: 1, core: 2. Of those that a mesh axis runs over, the one named last changes fastest.
Arguments:
- hidden: bfloat16 [16, 3072], P('dp')
- w_head: bfloat16 [3072, 256000], P(None, ('vblk', 'vocab'))
- inv_temp: float32 [16], P('dp')
- target: int32 [16], P('dp')
Outputs:
- output 1: float32 [16, 256000], P('dp', ('vblk', 'vocab'))
- output 2: float32 [16], P('dp')
All inputs are finite; a program needn't handle non-finite values.
Results may differ from the reference program's by a relative error of at most 0.001.
Values are sent between devices in bfloat16 or wider.
A program may use at most 1 GiB of HBM per device.

```python
import math
import jax
import jax.numpy as jnp
from jax import lax

D = 3072
V = 256000
ROWS = 16


def setup_inputs(seed: int = 0, part: int = 0) -> dict:
    root_key = jax.random.key(seed)
    key_dir, key_w = jax.random.split(root_key, 2)
    key_h, key_shift, key_temp, key_tgt = jax.random.split(jax.random.fold_in(root_key, part), 4)
    direction = jax.random.normal(key_dir, (D,), jnp.float32)
    direction = direction / jnp.sqrt(jnp.sum(direction * direction))

    def weight_block(block_idx):
        col_ids = (block_idx * 128 + jnp.arange(128)).astype(jnp.float32)
        col_gain = 40.0 + jnp.exp(-8.0 * col_ids / V)
        noise_blk = jax.random.normal(jax.random.fold_in(key_w, block_idx), (D, 128), jnp.float32)
        return (noise_blk * (1.5 / math.sqrt(D)) + direction[:, None] * col_gain[None, :]).astype(jnp.bfloat16)

    w_blocks = lax.map(weight_block, jnp.arange(V // 128))
    w_head = jnp.transpose(w_blocks, (1, 0, 2)).reshape(D, V)
    row_shift = jax.random.uniform(key_shift, (ROWS, 1), jnp.float32, 1.5, 3.5)
    hidden = (jax.random.normal(key_h, (ROWS, D), jnp.float32) + row_shift * direction[None, :]).astype(jnp.bfloat16)
    inv_temp = jax.random.uniform(key_temp, (ROWS,), jnp.float32, 0.75, 1.5)
    target = jax.random.randint(key_tgt, (ROWS,), 0, V, jnp.int32)
    target = target.at[0].set(0).at[ROWS - 1].set(V - 1)
    return {"hidden": hidden, "w_head": w_head, "inv_temp": inv_temp, "target": target}


def reference(hidden, w_head, inv_temp, target):
    logits = jnp.dot(hidden, w_head, preferred_element_type=jnp.float32) * inv_temp[:, None]
    row_max = jnp.max(logits, axis=1, keepdims=True)
    exp_val = jnp.exp(logits - row_max)
    prob_row = exp_val / jnp.sum(exp_val, axis=1, keepdims=True)
    cdf_table = jnp.cumsum(prob_row, axis=1)
    picked = jnp.take_along_axis(cdf_table, target[:, None], axis=1)[:, 0]
    return (cdf_table, picked)
```

```python
import functools

import jax
import jax.numpy as jnp
from jax import lax
from jax.experimental import pallas as pl
from jax.experimental.pallas import tpu as pltpu
from jax.sharding import PartitionSpec as P

MESH = pl.DeviceIdType.MESH
LANES = 128
GROUP = 256
TILE = 1024
TAPER = (512, 512, 256)
RING = 6


def stream_kernel(
    vblk_size, vocab_size, tau_hbm, tgt_hbm, h_hbm, w_hbm, c_ref, fin_ref,
    h_buf, w_buf, tri, run_max, pack, comm, tau_sm, tgt_sm, in_sem, w_sem, send_sem, recv_sem,
):
    n_dev = vblk_size * vocab_size
    rows = h_buf.shape[0]
    width = w_hbm.shape[1]
    n_full = (width - sum(TAPER)) // TILE
    me = lax.axis_index("vblk") * vocab_size + lax.axis_index("vocab")

    def peer_id(d):
        peer = lax.rem(me + d, n_dev)
        return {"vblk": lax.div(peer, vocab_size), "vocab": lax.rem(peer, vocab_size)}

    def w_copy(col, size, slot):
        return pltpu.make_async_copy(
            w_hbm.at[:, pl.ds(col, size)], w_buf.at[slot, :, pl.ds(0, size)], w_sem.at[slot]
        )

    small = [
        pltpu.make_async_copy(h_hbm, h_buf, in_sem.at[0]),
        pltpu.make_async_copy(tau_hbm, tau_sm, in_sem.at[1]),
        pltpu.make_async_copy(tgt_hbm, tgt_sm, in_sem.at[2]),
    ]
    for copy in small:
        copy.start()
    for t in range(RING):
        w_copy(t * TILE, TILE, t).start()

    barrier = pltpu.get_barrier_semaphore()
    for d in range(1, n_dev):
        pl.semaphore_signal(barrier, inc=1, device_id=peer_id(d), device_id_type=MESH)

    below = lax.broadcasted_iota(jnp.int32, tri.shape, 0)
    across = lax.broadcasted_iota(jnp.int32, tri.shape, 1)
    tri[...] = jnp.where((across >= GROUP) | (below <= across), 1.0, 0.0).astype(tri.dtype)

    for copy in small:
        copy.wait()
    row_id = lax.broadcasted_iota(jnp.int32, (rows, LANES), 0)
    lane_id = lax.broadcasted_iota(jnp.int32, (rows, LANES), 1)
    tau = jnp.zeros((rows, LANES), jnp.float32)
    tgt = jnp.zeros((rows, LANES), jnp.int32)
    for b in range(rows):
        tau = jnp.where(row_id == b, tau_sm[b], tau)
        tgt = jnp.where(row_id == b, tgt_sm[b], tgt)
    tgt_local = tgt - me * width

    def tile_step(index, col, size, slot, state):
        top, base, pick = state
        blocks, groups = size // LANES, size // GROUP
        z = jnp.dot(h_buf[...], w_buf[slot, :, pl.ds(0, size)], preferred_element_type=jnp.float32)
        z = [z[:, j * LANES:(j + 1) * LANES] * tau for j in range(blocks)]
        peak = functools.reduce(jnp.maximum, z)
        new_top = jnp.maximum(top, jnp.max(peak, axis=1, keepdims=True))
        alpha = jnp.exp(top - new_top)
        e = [jnp.exp(zj - new_top) for zj in z]
        e = jnp.concatenate([jnp.concatenate(e[2 * g:2 * g + 2], axis=1) for g in range(groups)], axis=0)
        hi = e.astype(jnp.bfloat16)
        rest = e - hi.astype(jnp.float32)
        mid = rest.astype(jnp.bfloat16)
        low = (rest - mid.astype(jnp.float32)).astype(jnp.bfloat16)
        sums = jnp.dot(jnp.concatenate([hi, mid, low], axis=0), tri[...], preferred_element_type=jnp.float32)
        n = rows * groups
        sums = sums[:n] + (sums[n:2 * n] + sums[2 * n:])
        base = base * alpha
        pick = pick * alpha
        hit = tgt_local - col
        for g in range(groups):
            part = sums[g * rows:(g + 1) * rows]
            for half in range(2):
                j = 2 * g + half
                value = part[:, half * LANES:(half + 1) * LANES] + base
                c_ref[:, pl.ds(col + j * LANES, LANES)] = value
                pick = pick + jnp.where(lane_id == hit - j * LANES, value, 0.0)
            base = base + part[:, GROUP:]
        run_max[index] = new_top
        return new_top, base, pick

    taper_cols = [n_full * TILE + sum(TAPER[:i]) for i in range(len(TAPER))]

    def full_step(t, state):
        slot = lax.rem(t, RING)
        w_copy(0, TILE, slot).wait()
        col = pl.multiple_of(t * TILE, TILE)
        state = tile_step(t, col, TILE, slot, state)

        @pl.when(t + RING < n_full)
        def _():
            w_copy(pl.multiple_of((t + RING) * TILE, TILE), TILE, slot).start()

        for i, (tcol, size) in enumerate(zip(taper_cols, TAPER)):
            @pl.when(t + RING == n_full + i)
            def _():
                w_copy(tcol, size, (n_full + i) % RING).start()

        return state

    zero = jnp.zeros((rows, LANES), jnp.float32)
    state = lax.fori_loop(0, n_full, full_step, (jnp.full((rows, LANES), -jnp.inf, jnp.float32), zero, zero))
    for i, (tcol, size) in enumerate(zip(taper_cols, TAPER)):
        slot = (n_full + i) % RING
        w_copy(tcol, size, slot).wait()
        state = tile_step(n_full + i, tcol, size, slot, state)
    top, total, pick = state

    diag = row_id == lane_id
    to_lanes = lambda x: jnp.sum(jnp.where(diag, x, 0.0), axis=0, keepdims=True)
    top_l = to_lanes(top)
    total_l = to_lanes(total)
    pick_l = to_lanes(jnp.broadcast_to(jnp.sum(pick, axis=1, keepdims=True), pick.shape))
    tgt_l = jnp.sum(jnp.where(diag, tgt, 0), axis=0, keepdims=True)
    sub = lax.broadcasted_iota(jnp.int32, (8, LANES), 0)
    packet = jnp.where(sub == 0, top_l, jnp.where(sub == 1, total_l, jnp.where(sub == 2, pick_l, 0.0)))
    pack[...] = packet
    comm[me] = packet

    pl.semaphore_wait(barrier, n_dev - 1)
    copies = [
        pltpu.make_async_remote_copy(
            src_ref=pack, dst_ref=comm.at[me], send_sem=send_sem.at[d - 1], recv_sem=recv_sem.at[d - 1],
            device_id=peer_id(d), device_id_type=MESH,
        )
        for d in range(1, n_dev)
    ]
    for copy in copies:
        copy.start()

    def rescale(index, col, size):
        factor = jnp.exp(run_max[index] - top)
        for j in range(size // LANES):
            cols = pl.ds(col + j * LANES, LANES)
            c_ref[:, cols] = c_ref[:, cols] * factor

    def rescale_full(t, carry):
        rescale(t, pl.multiple_of(t * TILE, TILE), TILE)
        return carry

    lax.fori_loop(0, n_full, rescale_full, 0)
    for i, (tcol, size) in enumerate(zip(taper_cols, TAPER)):
        rescale(n_full + i, tcol, size)

    for copy in copies:
        copy.wait()
    tops, sums, picks = comm[:, 0, :], comm[:, 1, :], comm[:, 2, :]
    top_all = jnp.max(tops, axis=0, keepdims=True)
    scale = jnp.exp(tops - top_all)
    mass = sums * scale
    dev = lax.broadcasted_iota(jnp.int32, (n_dev, LANES), 0)
    all_mass = jnp.sum(mass, axis=0, keepdims=True)
    lower = jnp.sum(jnp.where(dev < me, mass, 0.0), axis=0, keepdims=True)
    lower_tgt = jnp.sum(jnp.where((dev + 1) * width <= tgt_l, mass, 0.0), axis=0, keepdims=True)
    picked = jnp.sum(picks * scale, axis=0, keepdims=True) + lower_tgt
    mult = jnp.exp(top_l - top_all) / all_mass
    fin_ref[...] = jnp.where(
        sub == 0, mult, jnp.where(sub == 1, lower / all_mass, jnp.where(sub == 2, picked / all_mass, 0.0))
    )


def solution(mesh):
    vblk_size, vocab_size = mesh.shape["vblk"], mesh.shape["vocab"]
    n_dev = vblk_size * vocab_size

    def local_step(hidden, w_head, inv_temp, target):
        rows, depth = hidden.shape
        width = w_head.shape[1]
        n_tiles = (width - sum(TAPER)) // TILE + len(TAPER)
        hbm = pl.BlockSpec(memory_space=pltpu.HBM)
        vmem = pl.BlockSpec(memory_space=pltpu.VMEM)
        mass, fin = pl.pallas_call(
            functools.partial(stream_kernel, vblk_size, vocab_size),
            out_shape=(
                jax.ShapeDtypeStruct((rows, width), jnp.float32),
                jax.ShapeDtypeStruct((8, LANES), jnp.float32),
            ),
            in_specs=[hbm] * 4,
            out_specs=(vmem, vmem),
            scratch_shapes=[
                pltpu.VMEM((rows, depth), jnp.bfloat16),
                pltpu.VMEM((RING, depth, TILE), jnp.bfloat16),
                pltpu.VMEM((GROUP, GROUP + LANES), jnp.bfloat16),
                pltpu.VMEM((n_tiles, rows, LANES), jnp.float32),
                pltpu.VMEM((8, LANES), jnp.float32),
                pltpu.VMEM((n_dev, 8, LANES), jnp.float32),
                pltpu.SMEM((rows,), jnp.float32),
                pltpu.SMEM((rows,), jnp.int32),
                pltpu.SemaphoreType.DMA((3,)),
                pltpu.SemaphoreType.DMA((RING,)),
                pltpu.SemaphoreType.DMA((n_dev - 1,)),
                pltpu.SemaphoreType.DMA((n_dev - 1,)),
            ],
            compiler_params=pltpu.CompilerParams(
                collective_id=0, has_side_effects=True, vmem_limit_bytes=48 * 1024 * 1024
            ),
        )(*[pltpu.with_memory_space_constraint(x, pltpu.HBM) for x in (inv_temp, target, hidden, w_head)])
        cdf = mass * fin[0, :rows, None] + fin[1, :rows, None]
        return cdf, fin[2, :rows]

    vocab_axes = ("vblk", "vocab")
    return jax.shard_map(
        local_step,
        mesh=mesh,
        in_specs=(P("dp", None), P(None, vocab_axes), P("dp"), P("dp")),
        out_specs=(P("dp", vocab_axes), P("dp")),
        check_vma=False,
    )
```

```python
import functools

import jax
import jax.numpy as jnp
from jax import lax
from jax.experimental import pallas as pl
from jax.experimental.pallas import tpu as pltpu
from jax.sharding import PartitionSpec as P

MESH = pl.DeviceIdType.MESH
LANES = 128
GROUP = 256
TILE = 1280
CHUNKS = 6
RING = 3
PUSH = 512
PUSHES = 10
SLOTS = 4
OUT_CHUNKS = 5


def split_sums(e, tri):
    hi = e.astype(jnp.bfloat16)
    rest = e - hi.astype(jnp.float32)
    mid = rest.astype(jnp.bfloat16)
    low = (rest - mid.astype(jnp.float32)).astype(jnp.bfloat16)
    sums = jnp.dot(jnp.concatenate([hi, mid, low], axis=0), tri[...], preferred_element_type=jnp.float32)
    n = e.shape[0]
    return sums[:n] + (sums[n:2 * n] + sums[2 * n:])


def stream_kernel(
    vblk_size, vocab_size, tau_hbm, tgt_hbm, h_hbm, w_hbm, c_ref, fin_ref,
    h_buf, w_buf, push_buf, z_out, z_in, tri, near_max, far_max, far, pack, comm, tau_sm, tgt_sm,
    in_sem, w_sem, last_sem, push_send, push_recv, z_send, z_recv, send_sem, recv_sem,
):
    n_dev = vblk_size * vocab_size
    rows, depth = h_buf.shape
    width = w_hbm.shape[1]
    pushed = PUSH * PUSHES
    n_full = (width - pushed) // TILE - 1
    part = depth // CHUNKS
    vblk, vocab = lax.axis_index("vblk"), lax.axis_index("vocab")
    me = vblk * vocab_size + vocab
    chip, core = lax.div(vocab, 2), lax.rem(vocab, 2)
    sibling = {"vblk": vblk, "vocab": chip * 2 + (1 - core)}

    def peer_id(d):
        peer = lax.rem(me + d, n_dev)
        return {"vblk": lax.div(peer, vocab_size), "vocab": lax.rem(peer, vocab_size)}

    def near_col(t):
        return pl.multiple_of(pushed + t * TILE, LANES)

    def far_col(p):
        return pl.multiple_of(p * PUSH, LANES)

    def w_copy(t, slot):
        return pltpu.make_async_copy(w_hbm.at[:, pl.ds(near_col(t), TILE)], w_buf.at[slot], w_sem.at[slot])

    def last_copy(k):
        return pltpu.make_async_copy(
            w_hbm.at[pl.ds(k * part, part), pl.ds(near_col(n_full), TILE)],
            w_buf.at[n_full % RING, pl.ds(k * part, part)],
            last_sem.at[k],
        )

    def push_copy(p):
        return pltpu.make_async_remote_copy(
            src_ref=w_hbm.at[:, pl.ds(far_col(p), PUSH)], dst_ref=push_buf.at[p % SLOTS],
            send_sem=push_send.at[p], recv_sem=push_recv.at[p], device_id=sibling, device_id_type=MESH,
        )

    def z_copy(p):
        return pltpu.make_async_remote_copy(
            src_ref=z_out.at[p], dst_ref=z_in.at[p],
            send_sem=z_send.at[p], recv_sem=z_recv.at[p], device_id=sibling, device_id_type=MESH,
        )

    barrier = pltpu.get_barrier_semaphore()
    for d in range(1, n_dev):
        pl.semaphore_signal(barrier, inc=1, device_id=peer_id(d), device_id_type=MESH)

    small = [
        pltpu.make_async_copy(h_hbm, h_buf, in_sem.at[0]),
        pltpu.make_async_copy(tau_hbm, tau_sm, in_sem.at[1]),
        pltpu.make_async_copy(tgt_hbm, tgt_sm, in_sem.at[2]),
    ]
    for copy in small:
        copy.start()
    for t in range(RING):
        w_copy(t, t).start()

    pl.semaphore_wait(barrier, n_dev - 1)
    for p in range(2):
        push_copy(p).start()

    below = lax.broadcasted_iota(jnp.int32, tri.shape, 0)
    across = lax.broadcasted_iota(jnp.int32, tri.shape, 1)
    tri[...] = jnp.where((across >= GROUP) | (below <= across), 1.0, 0.0).astype(tri.dtype)

    for copy in small:
        copy.wait()
    row_id = lax.broadcasted_iota(jnp.int32, (rows, LANES), 0)
    lane_id = lax.broadcasted_iota(jnp.int32, (rows, LANES), 1)
    tau = jnp.zeros((rows, LANES), jnp.float32)
    tgt = jnp.zeros((rows, LANES), jnp.int32)
    for b in range(rows):
        tau = jnp.where(row_id == b, tau_sm[b], tau)
        tgt = jnp.where(row_id == b, tgt_sm[b], tgt)
    reach = tgt - me * width - lane_id

    def blocks_of(x):
        return [x[:, j * LANES:(j + 1) * LANES] for j in range(x.shape[1] // LANES)]

    def softmax_step(col, z, top, total, pick):
        z = [zj * tau for zj in blocks_of(z)]
        peak = functools.reduce(jnp.maximum, z)
        new_top = jnp.maximum(top, jnp.max(peak, axis=1, keepdims=True))
        alpha = jnp.exp(top - new_top)
        e = [jnp.exp(zj - new_top) for zj in z]
        total = total * alpha + functools.reduce(jnp.add, e)
        hit = reach - col
        pick = pick * alpha + functools.reduce(
            jnp.add, [jnp.where(hit >= j * LANES, ej, 0.0) for j, ej in enumerate(e)]
        )
        return e, alpha, new_top, total, pick

    def prefix_step(col, e, base):
        groups = len(e) * LANES // GROUP
        stacked = jnp.concatenate([jnp.concatenate(e[2 * g:2 * g + 2], axis=1) for g in range(groups)], axis=0)
        sums = split_sums(stacked, tri)
        for g in range(groups):
            part_sums = sums[g * rows:(g + 1) * rows]
            for half in range(2):
                c_ref[:, pl.ds(col + (2 * g + half) * LANES, LANES)] = (
                    part_sums[:, half * LANES:(half + 1) * LANES] + base
                )
            base = base + part_sums[:, GROUP:]
        return base

    far[0] = jnp.full((rows, LANES), -jnp.inf, jnp.float32)
    for i in range(1, 4):
        far[i] = jnp.zeros((rows, LANES), jnp.float32)

    def far_step(p):
        z_copy(p).wait_recv()
        e, alpha, top, total, pick = softmax_step(far_col(p), z_in[p], far[0], far[2], far[3])
        far[1] = prefix_step(far_col(p), e, far[1] * alpha)
        far[0], far[2], far[3] = top, total, pick
        far_max[p] = top

    def full_step(t, state):
        top, base, total, pick = state
        slot, odd, p = lax.rem(t, RING), lax.rem(t, 2), lax.div(t, 2)

        @pl.when(odd == 1)
        def _():
            push_copy(p).wait_recv()
            z_out[p] = jnp.dot(h_buf[...], push_buf[p % SLOTS], preferred_element_type=jnp.float32)

        w_copy(0, slot).wait()
        z = jnp.dot(h_buf[...], w_buf[slot], preferred_element_type=jnp.float32)

        @pl.when(t + RING < n_full)
        def _():
            w_copy(t + RING, slot).start()

        @pl.when(t + RING == n_full)
        def _():
            for k in range(CHUNKS):
                last_copy(k).start()

        @pl.when(odd == 1)
        def _():
            z_copy(p).start()

        @pl.when((odd == 1) & (p + 2 < PUSHES))
        def _():
            push_copy(p + 2).start()

        e, alpha, top, total, pick = softmax_step(near_col(t), z, top, total, pick)
        base = prefix_step(near_col(t), e, base * alpha)
        near_max[t] = top

        @pl.when((odd == 0) & (t >= 4))
        def _():
            far_step(p - 2)

        return top, base, total, pick

    zero = jnp.zeros((rows, LANES), jnp.float32)
    start = (jnp.full((rows, LANES), -jnp.inf, jnp.float32), zero, zero, zero)
    top, base, total, pick = lax.fori_loop(0, n_full, full_step, start)

    far_step(PUSHES - 2)
    far_step(PUSHES - 1)
    z = jnp.zeros((rows, TILE), jnp.float32)
    for k in range(CHUNKS):
        last_copy(k).wait()
        rows_k = pl.ds(k * part, part)
        z = z + jnp.dot(h_buf[:, rows_k], w_buf[n_full % RING, rows_k, :], preferred_element_type=jnp.float32)
    e, alpha, near_top, total, pick = softmax_step(near_col(n_full), z, top, total, pick)

    top = jnp.maximum(near_top, far[0])
    near_scale, far_scale = jnp.exp(near_top - top), jnp.exp(far[0] - top)
    diag = row_id == lane_id
    to_lanes = lambda x: jnp.sum(jnp.where(diag, x, 0.0), axis=0, keepdims=True)
    row_sum = lambda x: jnp.broadcast_to(jnp.sum(x, axis=1, keepdims=True), x.shape)
    top_l = to_lanes(top)
    total_l = to_lanes(row_sum(total * near_scale + far[2] * far_scale))
    pick_l = to_lanes(row_sum(pick * near_scale + far[3] * far_scale))
    sub = lax.broadcasted_iota(jnp.int32, (8, LANES), 0)
    packet = jnp.where(sub == 0, top_l, jnp.where(sub == 1, total_l, jnp.where(sub == 2, pick_l, 0.0)))
    pack[...] = packet
    comm[me] = packet

    copies = [
        pltpu.make_async_remote_copy(
            src_ref=pack, dst_ref=comm.at[me], send_sem=send_sem.at[d - 1], recv_sem=recv_sem.at[d - 1],
            device_id=peer_id(d), device_id_type=MESH,
        )
        for d in range(1, n_dev)
    ]
    for copy in copies:
        copy.start()

    prefix_step(near_col(n_full), e, base * alpha)
    near_max[n_full] = near_top
    far_sum = far[1] * far_scale

    def rescale_near(t, carry):
        factor = jnp.exp(near_max[t] - top)
        for j in range(TILE // LANES):
            cols = pl.ds(near_col(t) + j * LANES, LANES)
            c_ref[:, cols] = c_ref[:, cols] * factor + far_sum
        return carry

    def rescale_far(p, carry):
        factor = jnp.exp(far_max[p] - top)
        for j in range(PUSH // LANES):
            cols = pl.ds(far_col(p) + j * LANES, LANES)
            c_ref[:, cols] = c_ref[:, cols] * factor
        return carry

    lax.fori_loop(0, n_full + 1, rescale_near, 0)
    lax.fori_loop(0, PUSHES, rescale_far, 0)
    for p in range(PUSHES):
        push_copy(p).wait_send()
        z_copy(p).wait_send()

    for copy in copies:
        copy.wait()
    tops, sums, picks = comm[:, 0, :], comm[:, 1, :], comm[:, 2, :]
    top_all = jnp.max(tops, axis=0, keepdims=True)
    scale = jnp.exp(tops - top_all)
    mass = sums * scale
    dev = lax.broadcasted_iota(jnp.int32, (n_dev, LANES), 0)
    all_mass = jnp.sum(mass, axis=0, keepdims=True)
    lower = jnp.sum(jnp.where(dev < me, mass, 0.0), axis=0, keepdims=True)
    picked = jnp.sum(picks * scale, axis=0, keepdims=True)
    mult = jnp.exp(top_l - top_all) / all_mass
    fin_ref[...] = jnp.where(
        sub == 0, mult, jnp.where(sub == 1, lower / all_mass, jnp.where(sub == 2, picked / all_mass, 0.0))
    )


def finish_kernel(c_ref, fin_ref, cdf_hbm, picked_hbm, out_buf, picked_buf, out_sem):
    rows, width = c_ref.shape
    step = width // OUT_CHUNKS
    row_id = lax.broadcasted_iota(jnp.int32, (rows, LANES), 0)
    lane_id = lax.broadcasted_iota(jnp.int32, (rows, LANES), 1)
    fin = fin_ref[...]
    to_rows = lambda x: jnp.broadcast_to(
        jnp.sum(jnp.where(row_id == lane_id, x, 0.0), axis=1, keepdims=True), (rows, LANES)
    )
    mult, offset = to_rows(fin[0:1]), to_rows(fin[1:2])
    picked_buf[...] = fin[2, :rows]
    copies = [pltpu.make_async_copy(picked_buf, picked_hbm, out_sem.at[OUT_CHUNKS])]
    copies[0].start()
    for i in range(OUT_CHUNKS):
        for j in range(step // LANES):
            cols = pl.ds(i * step + j * LANES, LANES)
            out_buf[:, cols] = c_ref[:, cols] * mult + offset
        cols = pl.ds(i * step, step)
        copies.append(pltpu.make_async_copy(out_buf.at[:, cols], cdf_hbm.at[:, cols], out_sem.at[i]))
        copies[-1].start()
    for copy in copies:
        copy.wait()


def solution(mesh):
    vblk_size, vocab_size = mesh.shape["vblk"], mesh.shape["vocab"]
    n_dev = vblk_size * vocab_size

    def local_step(hidden, w_head, inv_temp, target):
        rows, depth = hidden.shape
        width = w_head.shape[1]
        hbm = pl.BlockSpec(memory_space=pltpu.HBM)
        vmem = pl.BlockSpec(memory_space=pltpu.VMEM)
        mass, fin = pl.pallas_call(
            functools.partial(stream_kernel, vblk_size, vocab_size),
            out_shape=(
                jax.ShapeDtypeStruct((rows, width), jnp.float32),
                jax.ShapeDtypeStruct((8, LANES), jnp.float32),
            ),
            in_specs=[hbm] * 4,
            out_specs=(vmem, vmem),
            scratch_shapes=[
                pltpu.VMEM((rows, depth), jnp.bfloat16),
                pltpu.VMEM((RING, depth, TILE), jnp.bfloat16),
                pltpu.VMEM((SLOTS, depth, PUSH), jnp.bfloat16),
                pltpu.VMEM((PUSHES, rows, PUSH), jnp.float32),
                pltpu.VMEM((PUSHES, rows, PUSH), jnp.float32),
                pltpu.VMEM((GROUP, GROUP + LANES), jnp.bfloat16),
                pltpu.VMEM(((width - PUSH * PUSHES) // TILE, rows, LANES), jnp.float32),
                pltpu.VMEM((PUSHES, rows, LANES), jnp.float32),
                pltpu.VMEM((4, rows, LANES), jnp.float32),
                pltpu.VMEM((8, LANES), jnp.float32),
                pltpu.VMEM((n_dev, 8, LANES), jnp.float32),
                pltpu.SMEM((rows,), jnp.float32),
                pltpu.SMEM((rows,), jnp.int32),
                pltpu.SemaphoreType.DMA((3,)),
                pltpu.SemaphoreType.DMA((RING,)),
                pltpu.SemaphoreType.DMA((CHUNKS,)),
                pltpu.SemaphoreType.DMA((PUSHES,)),
                pltpu.SemaphoreType.DMA((PUSHES,)),
                pltpu.SemaphoreType.DMA((PUSHES,)),
                pltpu.SemaphoreType.DMA((PUSHES,)),
                pltpu.SemaphoreType.DMA((n_dev - 1,)),
                pltpu.SemaphoreType.DMA((n_dev - 1,)),
            ],
            compiler_params=pltpu.CompilerParams(
                collective_id=0, has_side_effects=True, vmem_limit_bytes=44 * 1024 * 1024
            ),
        )(*[pltpu.with_memory_space_constraint(x, pltpu.HBM) for x in (inv_temp, target, hidden, w_head)])
        return pl.pallas_call(
            finish_kernel,
            out_shape=(
                jax.ShapeDtypeStruct((rows, width), jnp.float32),
                jax.ShapeDtypeStruct((rows,), jnp.float32),
            ),
            in_specs=[vmem, vmem],
            out_specs=(hbm, hbm),
            scratch_shapes=[
                pltpu.VMEM((rows, width), jnp.float32),
                pltpu.VMEM((rows,), jnp.float32),
                pltpu.SemaphoreType.DMA((OUT_CHUNKS + 1,)),
            ],
            compiler_params=pltpu.CompilerParams(vmem_limit_bytes=8 * 1024 * 1024),
        )(mass, fin)

    vocab_axes = ("vblk", "vocab")
    return jax.shard_map(
        local_step,
        mesh=mesh,
        in_specs=(P("dp", None), P(None, vocab_axes), P("dp"), P("dp")),
        out_specs=(P("dp", vocab_axes), P("dp")),
        check_vma=False,
    )
```

```python
import functools

import jax
import jax.numpy as jnp
from jax import lax
from jax.experimental import pallas as pl
from jax.experimental.pallas import tpu as pltpu
from jax.sharding import PartitionSpec as P

MESH = pl.DeviceIdType.MESH
LANES = 128
GROUP = 256
TILE = 1024
LAST = 1280
CHUNKS = (1536, 768, 512, 256)
RING = 4
PUSH = 512
PUSHES = 10
SLOTS = 4
OUT_CHUNKS = 5


def split_sums(e, tri):
    hi = e.astype(jnp.bfloat16)
    rest = e - hi.astype(jnp.float32)
    mid = rest.astype(jnp.bfloat16)
    low = (rest - mid.astype(jnp.float32)).astype(jnp.bfloat16)
    sums = jnp.dot(jnp.concatenate([hi, mid, low], axis=0), tri[...], preferred_element_type=jnp.float32)
    n = e.shape[0]
    return sums[:n] + (sums[n:2 * n] + sums[2 * n:])


def stream_kernel(
    vblk_size, vocab_size, tau_hbm, tgt_hbm, h_hbm, w_hbm, c_ref, fin_ref,
    h_buf, w_buf, last_buf, push_buf, z_out, z_in, z_late, z_last, tri, near_max, far_max, far, pack, comm, tau_sm, tgt_sm,
    ready, in_sem, w_sem, last_sem, push_send, push_recv, z_send, z_recv, send_sem, recv_sem,
):
    n_dev = vblk_size * vocab_size
    rows, depth = h_buf.shape
    width = w_hbm.shape[1]
    pushed = PUSH * PUSHES
    n_full = (width - pushed - LAST) // TILE
    last_col = width - LAST
    parts = [pl.ds(sum(CHUNKS[:k]), size) for k, size in enumerate(CHUNKS)]
    vblk, vocab = lax.axis_index("vblk"), lax.axis_index("vocab")
    me = vblk * vocab_size + vocab
    chip, core = lax.div(vocab, 2), lax.rem(vocab, 2)
    sibling = {"vblk": vblk, "vocab": chip * 2 + (1 - core)}

    def peer_id(d):
        peer = lax.rem(me + d, n_dev)
        return {"vblk": lax.div(peer, vocab_size), "vocab": lax.rem(peer, vocab_size)}

    def near_col(t):
        return pl.multiple_of(pushed + t * TILE, LANES)

    def far_col(p):
        return pl.multiple_of(p * PUSH, LANES)

    def w_copy(t, slot):
        return pltpu.make_async_copy(w_hbm.at[:, pl.ds(near_col(t), TILE)], w_buf.at[slot], w_sem.at[slot])

    def last_copy(k):
        return pltpu.make_async_copy(
            w_hbm.at[parts[k], pl.ds(last_col, LAST)], last_buf.at[parts[k]], last_sem.at[k]
        )

    def push_copy(p):
        return pltpu.make_async_remote_copy(
            src_ref=w_hbm.at[:, pl.ds(far_col(p), PUSH)], dst_ref=push_buf.at[p % SLOTS],
            send_sem=push_send.at[p], recv_sem=push_recv.at[p], device_id=sibling, device_id_type=MESH,
        )

    def z_copy(p):
        return pltpu.make_async_remote_copy(
            src_ref=z_out.at[p], dst_ref=z_in.at[p],
            send_sem=z_send.at[p], recv_sem=z_recv.at[p], device_id=sibling, device_id_type=MESH,
        )

    barrier = pltpu.get_barrier_semaphore()

    @pl.when(core == 0)
    def _():
        pl.semaphore_signal(barrier, inc=1, device_id=sibling, device_id_type=MESH)

    small = [
        pltpu.make_async_copy(h_hbm, h_buf, in_sem.at[0]),
        pltpu.make_async_copy(tau_hbm, tau_sm, in_sem.at[1]),
        pltpu.make_async_copy(tgt_hbm, tgt_sm, in_sem.at[2]),
    ]
    for copy in small:
        copy.start()
    for t in range(RING):
        w_copy(t, t).start()

    @pl.when(core == 1)
    def _():
        pl.semaphore_wait(barrier, 1)
        pl.semaphore_signal(ready, inc=1, device_id=sibling, device_id_type=MESH)

    @pl.when(core == 0)
    def _():
        pl.semaphore_wait(ready, 1)
        for d in range(2, n_dev, 2):
            pl.semaphore_signal(barrier, inc=1, device_id=peer_id(d), device_id_type=MESH)

    for p in range(2):
        push_copy(p).start()

    below = lax.broadcasted_iota(jnp.int32, tri.shape, 0)
    across = lax.broadcasted_iota(jnp.int32, tri.shape, 1)
    tri[...] = jnp.where((across >= GROUP) | (below <= across), 1.0, 0.0).astype(tri.dtype)

    for copy in small:
        copy.wait()
    row_id = lax.broadcasted_iota(jnp.int32, (rows, LANES), 0)
    lane_id = lax.broadcasted_iota(jnp.int32, (rows, LANES), 1)
    tau = jnp.zeros((rows, LANES), jnp.float32)
    tgt = jnp.zeros((rows, LANES), jnp.int32)
    for b in range(rows):
        tau = jnp.where(row_id == b, tau_sm[b], tau)
        tgt = jnp.where(row_id == b, tgt_sm[b], tgt)
    reach = tgt - me * width - lane_id

    def blocks_of(x):
        return [x[:, j * LANES:(j + 1) * LANES] for j in range(x.shape[1] // LANES)]

    def softmax_step(col, z, top, total, pick):
        z = [zj * tau for zj in blocks_of(z)]
        peak = functools.reduce(jnp.maximum, z)
        new_top = jnp.maximum(top, jnp.max(peak, axis=1, keepdims=True))
        alpha = jnp.exp(top - new_top)
        e = [jnp.exp(zj - new_top) for zj in z]
        total = total * alpha + functools.reduce(jnp.add, e)
        hit = reach - col
        pick = pick * alpha + functools.reduce(
            jnp.add, [jnp.where(hit >= j * LANES, ej, 0.0) for j, ej in enumerate(e)]
        )
        return e, alpha, new_top, total, pick

    def prefix_step(col, e, base):
        groups = len(e) * LANES // GROUP
        stacked = jnp.concatenate([jnp.concatenate(e[2 * g:2 * g + 2], axis=1) for g in range(groups)], axis=0)
        sums = split_sums(stacked, tri)
        for g in range(groups):
            part_sums = sums[g * rows:(g + 1) * rows]
            for half in range(2):
                c_ref[:, pl.ds(col + (2 * g + half) * LANES, LANES)] = (
                    part_sums[:, half * LANES:(half + 1) * LANES] + base
                )
            base = base + part_sums[:, GROUP:]
        return base

    far[0] = jnp.full((rows, LANES), -jnp.inf, jnp.float32)
    for i in range(1, 4):
        far[i] = jnp.zeros((rows, LANES), jnp.float32)

    def far_step(p):
        z_copy(p).wait_recv()
        e, alpha, top, total, pick = softmax_step(far_col(p), z_in[p], far[0], far[2], far[3])
        far[1] = prefix_step(far_col(p), e, far[1] * alpha)
        far[0], far[2], far[3] = top, total, pick
        far_max[p] = top

    def near_step(t, z, state):
        top, base, total, pick = state
        e, alpha, top, total, pick = softmax_step(near_col(t), z, top, total, pick)
        base = prefix_step(near_col(t), e, base * alpha)
        near_max[t] = top
        return top, base, total, pick

    def near_dot(t):
        slot = lax.rem(t, RING)
        w_copy(0, slot).wait()
        return jnp.dot(h_buf[...], w_buf[slot], preferred_element_type=jnp.float32)

    def refill(t):
        @pl.when(t + RING < n_full)
        def _():
            w_copy(t + RING, lax.rem(t, RING)).start()

        @pl.when(t + RING == n_full)
        def _():
            for k in range(len(CHUNKS)):
                last_copy(k).start()

    def push_dot(p):
        push_copy(p).wait_recv()
        z_out[p] = jnp.dot(h_buf[...], push_buf[lax.rem(p, SLOTS)], preferred_element_type=jnp.float32)

    def answer(p):
        z_copy(p).start()

        @pl.when(p + 2 < PUSHES)
        def _():
            push_copy(p + 2).start()

    def round_step(u, state, first=False):
        t, p = 5 * u, 2 * u
        z = near_dot(t)
        if not first:
            state = near_step(t - 1, z_late[...], state)
            far_step(p - 2)
        refill(t)
        z_next = near_dot(t + 1)
        state = near_step(t, z, state)
        refill(t + 1)
        z = near_dot(t + 2)
        state = near_step(t + 1, z_next, state)
        refill(t + 2)
        push_dot(p)
        z_next = near_dot(t + 3)
        state = near_step(t + 2, z, state)
        answer(p)
        if not first:
            far_step(p - 1)
        refill(t + 3)
        z = near_dot(t + 4)
        z_late[...] = z
        refill(t + 4)
        push_dot(p + 1)
        state = near_step(t + 3, z_next, state)
        answer(p + 1)
        return state

    zero = jnp.zeros((rows, LANES), jnp.float32)
    state = (jnp.full((rows, LANES), -jnp.inf, jnp.float32), zero, zero, zero)
    state = round_step(jnp.int32(0), state, first=True)
    state = lax.fori_loop(1, n_full // 5, round_step, state)

    @pl.when(core == 0)
    def _():
        pl.semaphore_wait(barrier, n_dev // 2 - 1)
        pl.semaphore_signal(ready, inc=1, device_id=sibling, device_id_type=MESH)

    def last_dot(k):
        last_copy(k).wait()
        return jnp.dot(h_buf[:, parts[k]], last_buf[parts[k], :], preferred_element_type=jnp.float32)

    z_last[...] = last_dot(0)
    top, base, total, pick = near_step(n_full - 1, z_late[...], state)
    far_step(PUSHES - 2)
    z_last[...] += last_dot(1)
    far_step(PUSHES - 1)
    z = z_last[...]
    for k in range(2, len(CHUNKS)):
        z = z + last_dot(k)
    e, alpha, near_top, total, pick = softmax_step(last_col, z, top, total, pick)

    top = jnp.maximum(near_top, far[0])
    near_scale, far_scale = jnp.exp(near_top - top), jnp.exp(far[0] - top)
    diag = row_id == lane_id
    to_lanes = lambda x: jnp.sum(jnp.where(diag, x, 0.0), axis=0, keepdims=True)
    row_sum = lambda x: jnp.broadcast_to(jnp.sum(x, axis=1, keepdims=True), x.shape)
    top_l = to_lanes(top)
    total_l = to_lanes(row_sum(total * near_scale + far[2] * far_scale))
    pick_l = to_lanes(row_sum(pick * near_scale + far[3] * far_scale))
    sub = lax.broadcasted_iota(jnp.int32, (8, LANES), 0)
    packet = jnp.where(sub == 0, top_l, jnp.where(sub == 1, total_l, jnp.where(sub == 2, pick_l, 0.0)))
    pack[...] = packet
    comm[me] = packet

    @pl.when(core == 1)
    def _():
        pl.semaphore_wait(ready, 1)

    copies = [
        pltpu.make_async_remote_copy(
            src_ref=pack, dst_ref=comm.at[me], send_sem=send_sem.at[d - 1], recv_sem=recv_sem.at[d - 1],
            device_id=peer_id(d), device_id_type=MESH,
        )
        for d in range(1, n_dev)
    ]
    for copy in copies:
        copy.start()

    prefix_step(last_col, e, base * alpha)
    far_sum = far[1] * far_scale

    def rescale_near(t, carry):
        factor = jnp.exp(near_max[t] - top)
        for j in range(TILE // LANES):
            cols = pl.ds(near_col(t) + j * LANES, LANES)
            c_ref[:, cols] = c_ref[:, cols] * factor + far_sum
        return carry

    def rescale_far(p, carry):
        factor = jnp.exp(far_max[p] - top)
        for j in range(PUSH // LANES):
            cols = pl.ds(far_col(p) + j * LANES, LANES)
            c_ref[:, cols] = c_ref[:, cols] * factor
        return carry

    lax.fori_loop(0, n_full, rescale_near, 0)
    for j in range(LAST // LANES):
        cols = pl.ds(last_col + j * LANES, LANES)
        c_ref[:, cols] = c_ref[:, cols] * near_scale + far_sum
    lax.fori_loop(0, PUSHES, rescale_far, 0)
    for p in range(PUSHES):
        push_copy(p).wait_send()
        z_copy(p).wait_send()

    for copy in copies:
        copy.wait()
    tops, sums, picks = comm[:, 0, :], comm[:, 1, :], comm[:, 2, :]
    top_all = jnp.max(tops, axis=0, keepdims=True)
    scale = jnp.exp(tops - top_all)
    mass = sums * scale
    dev = lax.broadcasted_iota(jnp.int32, (n_dev, LANES), 0)
    all_mass = jnp.sum(mass, axis=0, keepdims=True)
    lower = jnp.sum(jnp.where(dev < me, mass, 0.0), axis=0, keepdims=True)
    picked = jnp.sum(picks * scale, axis=0, keepdims=True)
    mult = jnp.exp(top_l - top_all) / all_mass
    fin_ref[...] = jnp.where(
        sub == 0, mult, jnp.where(sub == 1, lower / all_mass, jnp.where(sub == 2, picked / all_mass, 0.0))
    )


def finish_kernel(c_ref, fin_ref, cdf_hbm, picked_hbm, out_buf, picked_buf, out_sem):
    rows, width = c_ref.shape
    step = width // OUT_CHUNKS
    row_id = lax.broadcasted_iota(jnp.int32, (rows, LANES), 0)
    lane_id = lax.broadcasted_iota(jnp.int32, (rows, LANES), 1)
    fin = fin_ref[...]
    to_rows = lambda x: jnp.broadcast_to(
        jnp.sum(jnp.where(row_id == lane_id, x, 0.0), axis=1, keepdims=True), (rows, LANES)
    )
    mult, offset = to_rows(fin[0:1]), to_rows(fin[1:2])
    picked_buf[...] = fin[2, :rows]
    copies = [pltpu.make_async_copy(picked_buf, picked_hbm, out_sem.at[OUT_CHUNKS])]
    copies[0].start()
    for i in range(OUT_CHUNKS):
        for j in range(step // LANES):
            cols = pl.ds(i * step + j * LANES, LANES)
            out_buf[:, cols] = c_ref[:, cols] * mult + offset
        cols = pl.ds(i * step, step)
        copies.append(pltpu.make_async_copy(out_buf.at[:, cols], cdf_hbm.at[:, cols], out_sem.at[i]))
        copies[-1].start()
    for copy in copies:
        copy.wait()


def solution(mesh):
    vblk_size, vocab_size = mesh.shape["vblk"], mesh.shape["vocab"]
    n_dev = vblk_size * vocab_size

    def local_step(hidden, w_head, inv_temp, target):
        rows, depth = hidden.shape
        width = w_head.shape[1]
        hbm = pl.BlockSpec(memory_space=pltpu.HBM)
        vmem = pl.BlockSpec(memory_space=pltpu.VMEM)
        mass, fin = pl.pallas_call(
            functools.partial(stream_kernel, vblk_size, vocab_size),
            out_shape=(
                jax.ShapeDtypeStruct((rows, width), jnp.float32),
                jax.ShapeDtypeStruct((8, LANES), jnp.float32),
            ),
            in_specs=[hbm] * 4,
            out_specs=(vmem, vmem),
            scratch_shapes=[
                pltpu.VMEM((rows, depth), jnp.bfloat16),
                pltpu.VMEM((RING, depth, TILE), jnp.bfloat16),
                pltpu.VMEM((depth, LAST), jnp.bfloat16),
                pltpu.VMEM((SLOTS, depth, PUSH), jnp.bfloat16),
                pltpu.VMEM((PUSHES, rows, PUSH), jnp.float32),
                pltpu.VMEM((PUSHES, rows, PUSH), jnp.float32),
                pltpu.VMEM((rows, TILE), jnp.float32),
                pltpu.VMEM((rows, LAST), jnp.float32),
                pltpu.VMEM((GROUP, GROUP + LANES), jnp.bfloat16),
                pltpu.VMEM(((width - PUSH * PUSHES - LAST) // TILE, rows, LANES), jnp.float32),
                pltpu.VMEM((PUSHES, rows, LANES), jnp.float32),
                pltpu.VMEM((4, rows, LANES), jnp.float32),
                pltpu.VMEM((8, LANES), jnp.float32),
                pltpu.VMEM((n_dev, 8, LANES), jnp.float32),
                pltpu.SMEM((rows,), jnp.float32),
                pltpu.SMEM((rows,), jnp.int32),
                pltpu.SemaphoreType.REGULAR,
                pltpu.SemaphoreType.DMA((3,)),
                pltpu.SemaphoreType.DMA((RING,)),
                pltpu.SemaphoreType.DMA((len(CHUNKS),)),
                pltpu.SemaphoreType.DMA((PUSHES,)),
                pltpu.SemaphoreType.DMA((PUSHES,)),
                pltpu.SemaphoreType.DMA((PUSHES,)),
                pltpu.SemaphoreType.DMA((PUSHES,)),
                pltpu.SemaphoreType.DMA((n_dev - 1,)),
                pltpu.SemaphoreType.DMA((n_dev - 1,)),
            ],
            compiler_params=pltpu.CompilerParams(
                collective_id=0, has_side_effects=True, vmem_limit_bytes=48 * 1024 * 1024
            ),
        )(*[pltpu.with_memory_space_constraint(x, pltpu.HBM) for x in (inv_temp, target, hidden, w_head)])
        return pl.pallas_call(
            finish_kernel,
            out_shape=(
                jax.ShapeDtypeStruct((rows, width), jnp.float32),
                jax.ShapeDtypeStruct((rows,), jnp.float32),
            ),
            in_specs=[vmem, vmem],
            out_specs=(hbm, hbm),
            scratch_shapes=[
                pltpu.VMEM((rows, width), jnp.float32),
                pltpu.VMEM((rows,), jnp.float32),
                pltpu.SemaphoreType.DMA((OUT_CHUNKS + 1,)),
            ],
            compiler_params=pltpu.CompilerParams(vmem_limit_bytes=8 * 1024 * 1024),
        )(mass, fin)

    vocab_axes = ("vblk", "vocab")
    return jax.shard_map(
        local_step,
        mesh=mesh,
        in_specs=(P("dp", None), P(None, vocab_axes), P("dp"), P("dp")),
        out_specs=(P("dp", vocab_axes), P("dp")),
        check_vma=False,
    )
```

```python
import functools

import jax
import jax.numpy as jnp
from jax import lax
from jax.experimental import pallas as pl
from jax.experimental.pallas import tpu as pltpu
from jax.sharding import PartitionSpec as P

MESH = pl.DeviceIdType.MESH
LANES = 128
GROUP = 256
TILE = 1024
LAST = 1280
CHUNKS = (1536, 768, 512, 256)
RING = 4
PUSH = 512
PUSHES = 10
SLOTS = 4
OUT_CHUNKS = 5


def split_sums(e, tri):
    hi = e.astype(jnp.bfloat16)
    rest = e - hi.astype(jnp.float32)
    mid = rest.astype(jnp.bfloat16)
    low = (rest - mid.astype(jnp.float32)).astype(jnp.bfloat16)
    sums = jnp.dot(jnp.concatenate([hi, mid, low], axis=0), tri[...], preferred_element_type=jnp.float32)
    n = e.shape[0]
    return sums[:n] + (sums[n:2 * n] + sums[2 * n:])


def stream_kernel(
    vblk_size, vocab_size, tau_hbm, tgt_hbm, h_hbm, w_hbm, c_ref, fin_ref,
    h_buf, w_buf, last_buf, push_buf, z_out, z_in, z_late, z_last, tri, near_max, far_max, far, guest, pack, comm, tau_sm, tgt_sm,
    ready, in_sem, w_sem, last_sem, push_send, push_recv, z_send, z_recv, send_sem, recv_sem,
):
    n_dev = vblk_size * vocab_size
    rows, depth = h_buf.shape
    width = w_hbm.shape[1]
    pushed = PUSH * PUSHES
    n_full = (width - pushed - LAST) // TILE
    last_col = width - LAST
    parts = [pl.ds(sum(CHUNKS[:k]), size) for k, size in enumerate(CHUNKS)]
    vblk, vocab = lax.axis_index("vblk"), lax.axis_index("vocab")
    me = vblk * vocab_size + vocab
    chip, core = lax.div(vocab, 2), lax.rem(vocab, 2)
    sibling = {"vblk": vblk, "vocab": chip * 2 + (1 - core)}

    def peer_id(d):
        peer = lax.rem(me + d, n_dev)
        return {"vblk": lax.div(peer, vocab_size), "vocab": lax.rem(peer, vocab_size)}

    def near_col(t):
        return pl.multiple_of(pushed + t * TILE, LANES)

    def far_col(p):
        return pl.multiple_of(p * PUSH, LANES)

    def w_copy(t, slot):
        return pltpu.make_async_copy(w_hbm.at[:, pl.ds(near_col(t), TILE)], w_buf.at[slot], w_sem.at[slot])

    def last_copy(k):
        return pltpu.make_async_copy(
            w_hbm.at[parts[k], pl.ds(last_col, LAST)], last_buf.at[parts[k]], last_sem.at[k]
        )

    def push_copy(p):
        return pltpu.make_async_remote_copy(
            src_ref=w_hbm.at[:, pl.ds(far_col(p), PUSH)], dst_ref=push_buf.at[p % SLOTS],
            send_sem=push_send.at[p], recv_sem=push_recv.at[p], device_id=sibling, device_id_type=MESH,
        )

    def z_copy(p):
        return pltpu.make_async_remote_copy(
            src_ref=z_out.at[p], dst_ref=z_in.at[p],
            send_sem=z_send.at[p], recv_sem=z_recv.at[p], device_id=sibling, device_id_type=MESH,
        )

    barrier = pltpu.get_barrier_semaphore()

    @pl.when(core == 0)
    def _():
        pl.semaphore_signal(barrier, inc=1, device_id=sibling, device_id_type=MESH)

    small = [
        pltpu.make_async_copy(h_hbm, h_buf, in_sem.at[0]),
        pltpu.make_async_copy(tau_hbm, tau_sm, in_sem.at[1]),
        pltpu.make_async_copy(tgt_hbm, tgt_sm, in_sem.at[2]),
    ]
    for copy in small:
        copy.start()
    for t in range(RING):
        w_copy(t, t).start()

    @pl.when(core == 1)
    def _():
        pl.semaphore_wait(barrier, 1)
        pl.semaphore_signal(ready, inc=1, device_id=sibling, device_id_type=MESH)

    @pl.when(core == 0)
    def _():
        pl.semaphore_wait(ready, 1)
        for d in range(2, n_dev, 2):
            pl.semaphore_signal(barrier, inc=1, device_id=peer_id(d), device_id_type=MESH)

    for p in range(2):
        push_copy(p).start()

    below = lax.broadcasted_iota(jnp.int32, tri.shape, 0)
    across = lax.broadcasted_iota(jnp.int32, tri.shape, 1)
    tri[...] = jnp.where((across >= GROUP) | (below <= across), 1.0, 0.0).astype(tri.dtype)

    for copy in small:
        copy.wait()
    row_id = lax.broadcasted_iota(jnp.int32, (rows, LANES), 0)
    lane_id = lax.broadcasted_iota(jnp.int32, (rows, LANES), 1)
    tau = jnp.zeros((rows, LANES), jnp.float32)
    tgt = jnp.zeros((rows, LANES), jnp.int32)
    for b in range(rows):
        tau = jnp.where(row_id == b, tau_sm[b], tau)
        tgt = jnp.where(row_id == b, tgt_sm[b], tgt)
    reach = tgt - me * width - lane_id
    host = vblk * vocab_size + chip * 2 + (1 - core)
    guest_reach = tgt - host * width - lane_id

    def blocks_of(x):
        return [x[:, j * LANES:(j + 1) * LANES] for j in range(x.shape[1] // LANES)]

    def softmax_step(col, z, top, total, pick, reach=reach):
        z = [zj * tau for zj in blocks_of(z)]
        peak = functools.reduce(jnp.maximum, z)
        new_top = jnp.maximum(top, jnp.max(peak, axis=1, keepdims=True))
        alpha = jnp.exp(top - new_top)
        e = [jnp.exp(zj - new_top) for zj in z]
        total = total * alpha + functools.reduce(jnp.add, e)
        hit = reach - col
        pick = pick * alpha + functools.reduce(
            jnp.add, [jnp.where(hit >= j * LANES, ej, 0.0) for j, ej in enumerate(e)]
        )
        return e, alpha, new_top, total, pick

    def prefix_step(col, e, base):
        groups = len(e) * LANES // GROUP
        stacked = jnp.concatenate([jnp.concatenate(e[2 * g:2 * g + 2], axis=1) for g in range(groups)], axis=0)
        sums = split_sums(stacked, tri)
        for g in range(groups):
            part_sums = sums[g * rows:(g + 1) * rows]
            for half in range(2):
                c_ref[:, pl.ds(col + (2 * g + half) * LANES, LANES)] = (
                    part_sums[:, half * LANES:(half + 1) * LANES] + base
                )
            base = base + part_sums[:, GROUP:]
        return base

    lowest, zero = jnp.full((rows, LANES), -jnp.inf, jnp.float32), jnp.zeros((rows, LANES), jnp.float32)
    far[0], far[1] = lowest, zero
    guest[0], guest[1], guest[2] = lowest, zero, zero

    def far_step(p):
        z_copy(p).wait_recv()
        e, alpha, top, _, _ = softmax_step(far_col(p), z_in[p], far[0], zero, zero)
        far[1] = prefix_step(far_col(p), e, far[1] * alpha)
        far[0] = top
        far_max[p] = top

    def near_step(t, z, state):
        top, base, total, pick = state
        e, alpha, top, total, pick = softmax_step(near_col(t), z, top, total, pick)
        base = prefix_step(near_col(t), e, base * alpha)
        near_max[t] = top
        return top, base, total, pick

    def near_dot(t):
        slot = lax.rem(t, RING)
        w_copy(0, slot).wait()
        return jnp.dot(h_buf[...], w_buf[slot], preferred_element_type=jnp.float32)

    def refill(t):
        @pl.when(t + RING < n_full)
        def _():
            w_copy(t + RING, lax.rem(t, RING)).start()

        @pl.when(t + RING == n_full)
        def _():
            for k in range(len(CHUNKS)):
                last_copy(k).start()

    def push_dot(p):
        push_copy(p).wait_recv()
        z = jnp.dot(h_buf[...], push_buf[lax.rem(p, SLOTS)], preferred_element_type=jnp.float32)
        z_out[p] = z
        _, _, guest[0], guest[1], guest[2] = softmax_step(far_col(p), z, guest[0], guest[1], guest[2], guest_reach)

    def answer(p):
        z_copy(p).start()

        @pl.when(p + 2 < PUSHES)
        def _():
            push_copy(p + 2).start()

    def round_step(u, state, first=False):
        t, p = 5 * u, 2 * u
        z = near_dot(t)
        if not first:
            state = near_step(t - 1, z_late[...], state)
            far_step(p - 2)
        refill(t)
        z_next = near_dot(t + 1)
        state = near_step(t, z, state)
        refill(t + 1)
        z = near_dot(t + 2)
        state = near_step(t + 1, z_next, state)
        refill(t + 2)
        push_dot(p)
        z_next = near_dot(t + 3)
        state = near_step(t + 2, z, state)
        answer(p)
        if not first:
            far_step(p - 1)
        refill(t + 3)
        z = near_dot(t + 4)
        z_late[...] = z
        refill(t + 4)
        push_dot(p + 1)
        state = near_step(t + 3, z_next, state)
        answer(p + 1)
        return state

    state = (lowest, zero, zero, zero)
    state = round_step(jnp.int32(0), state, first=True)
    state = lax.fori_loop(1, n_full // 5, round_step, state)

    @pl.when(core == 0)
    def _():
        pl.semaphore_wait(barrier, n_dev // 2 - 1)
        pl.semaphore_signal(ready, inc=1, device_id=sibling, device_id_type=MESH)

    def last_dot(k):
        last_copy(k).wait()
        return jnp.dot(h_buf[:, parts[k]], last_buf[parts[k], :], preferred_element_type=jnp.float32)

    z_last[...] = last_dot(0)
    top, base, total, pick = near_step(n_full - 1, z_late[...], state)
    z_last[...] += last_dot(1)
    z = z_last[...]
    for k in range(2, len(CHUNKS)):
        z = z + last_dot(k)
    e, alpha, near_top, total, pick = softmax_step(last_col, z, top, total, pick)

    diag = row_id == lane_id
    to_lanes = lambda x: jnp.sum(jnp.where(diag, x, 0.0), axis=0, keepdims=True)
    row_sum = lambda x: jnp.broadcast_to(jnp.sum(x, axis=1, keepdims=True), x.shape)
    sub = lax.broadcasted_iota(jnp.int32, (8, LANES), 0)
    packet = jnp.zeros((8, LANES), jnp.float32)
    stats = (near_top, row_sum(total), row_sum(pick), guest[0], row_sum(guest[1]), row_sum(guest[2]))
    for i, stat in enumerate(stats):
        packet = jnp.where(sub == i, to_lanes(stat), packet)
    pack[...] = packet
    comm[me] = packet

    @pl.when(core == 1)
    def _():
        pl.semaphore_wait(ready, 1)

    copies = [
        pltpu.make_async_remote_copy(
            src_ref=pack, dst_ref=comm.at[me], send_sem=send_sem.at[d - 1], recv_sem=recv_sem.at[d - 1],
            device_id=peer_id(d), device_id_type=MESH,
        )
        for d in range(1, n_dev)
    ]
    for copy in copies:
        copy.start()

    far_step(PUSHES - 2)
    far_step(PUSHES - 1)
    top = jnp.maximum(near_top, far[0])
    near_scale, far_scale = jnp.exp(near_top - top), jnp.exp(far[0] - top)
    prefix_step(last_col, e, base * alpha)
    far_sum = far[1] * far_scale

    def rescale_near(t, carry):
        factor = jnp.exp(near_max[t] - top)
        for j in range(TILE // LANES):
            cols = pl.ds(near_col(t) + j * LANES, LANES)
            c_ref[:, cols] = c_ref[:, cols] * factor + far_sum
        return carry

    def rescale_far(p, carry):
        factor = jnp.exp(far_max[p] - top)
        for j in range(PUSH // LANES):
            cols = pl.ds(far_col(p) + j * LANES, LANES)
            c_ref[:, cols] = c_ref[:, cols] * factor
        return carry

    lax.fori_loop(0, n_full, rescale_near, 0)
    for j in range(LAST // LANES):
        cols = pl.ds(last_col + j * LANES, LANES)
        c_ref[:, cols] = c_ref[:, cols] * near_scale + far_sum
    lax.fori_loop(0, PUSHES, rescale_far, 0)
    for p in range(PUSHES):
        push_copy(p).wait_send()
        z_copy(p).wait_send()

    for copy in copies:
        copy.wait()
    dev = lax.broadcasted_iota(jnp.int32, (n_dev, LANES), 0)
    hosts = dev + 1 - 2 * lax.rem(dev, 2)
    tops, guest_tops = comm[:, 0, :], comm[:, 3, :]
    top_all = jnp.max(jnp.maximum(tops, guest_tops), axis=0, keepdims=True)
    scale, guest_scale = jnp.exp(tops - top_all), jnp.exp(guest_tops - top_all)
    mass, guest_mass = comm[:, 1, :] * scale, comm[:, 4, :] * guest_scale
    all_mass = jnp.sum(mass + guest_mass, axis=0, keepdims=True)
    lower = jnp.sum(jnp.where(dev < me, mass, 0.0) + jnp.where(hosts < me, guest_mass, 0.0), axis=0, keepdims=True)
    picked = jnp.sum(comm[:, 2, :] * scale + comm[:, 5, :] * guest_scale, axis=0, keepdims=True)
    mult = jnp.exp(to_lanes(top) - top_all) / all_mass
    fin_ref[...] = jnp.where(
        sub == 0, mult, jnp.where(sub == 1, lower / all_mass, jnp.where(sub == 2, picked / all_mass, 0.0))
    )


def finish_kernel(c_ref, fin_ref, cdf_hbm, picked_hbm, out_buf, picked_buf, out_sem):
    rows, width = c_ref.shape
    step = width // OUT_CHUNKS
    row_id = lax.broadcasted_iota(jnp.int32, (rows, LANES), 0)
    lane_id = lax.broadcasted_iota(jnp.int32, (rows, LANES), 1)
    fin = fin_ref[...]
    to_rows = lambda x: jnp.broadcast_to(
        jnp.sum(jnp.where(row_id == lane_id, x, 0.0), axis=1, keepdims=True), (rows, LANES)
    )
    mult, offset = to_rows(fin[0:1]), to_rows(fin[1:2])
    picked_buf[...] = fin[2, :rows]
    copies = [pltpu.make_async_copy(picked_buf, picked_hbm, out_sem.at[OUT_CHUNKS])]
    copies[0].start()
    for i in range(OUT_CHUNKS):
        for j in range(step // LANES):
            cols = pl.ds(i * step + j * LANES, LANES)
            out_buf[:, cols] = c_ref[:, cols] * mult + offset
        cols = pl.ds(i * step, step)
        copies.append(pltpu.make_async_copy(out_buf.at[:, cols], cdf_hbm.at[:, cols], out_sem.at[i]))
        copies[-1].start()
    for copy in copies:
        copy.wait()


def solution(mesh):
    vblk_size, vocab_size = mesh.shape["vblk"], mesh.shape["vocab"]
    n_dev = vblk_size * vocab_size

    def local_step(hidden, w_head, inv_temp, target):
        rows, depth = hidden.shape
        width = w_head.shape[1]
        hbm = pl.BlockSpec(memory_space=pltpu.HBM)
        vmem = pl.BlockSpec(memory_space=pltpu.VMEM)
        mass, fin = pl.pallas_call(
            functools.partial(stream_kernel, vblk_size, vocab_size),
            out_shape=(
                jax.ShapeDtypeStruct((rows, width), jnp.float32),
                jax.ShapeDtypeStruct((8, LANES), jnp.float32),
            ),
            in_specs=[hbm] * 4,
            out_specs=(vmem, vmem),
            scratch_shapes=[
                pltpu.VMEM((rows, depth), jnp.bfloat16),
                pltpu.VMEM((RING, depth, TILE), jnp.bfloat16),
                pltpu.VMEM((depth, LAST), jnp.bfloat16),
                pltpu.VMEM((SLOTS, depth, PUSH), jnp.bfloat16),
                pltpu.VMEM((PUSHES, rows, PUSH), jnp.float32),
                pltpu.VMEM((PUSHES, rows, PUSH), jnp.float32),
                pltpu.VMEM((rows, TILE), jnp.float32),
                pltpu.VMEM((rows, LAST), jnp.float32),
                pltpu.VMEM((GROUP, GROUP + LANES), jnp.bfloat16),
                pltpu.VMEM(((width - PUSH * PUSHES - LAST) // TILE, rows, LANES), jnp.float32),
                pltpu.VMEM((PUSHES, rows, LANES), jnp.float32),
                pltpu.VMEM((2, rows, LANES), jnp.float32),
                pltpu.VMEM((3, rows, LANES), jnp.float32),
                pltpu.VMEM((8, LANES), jnp.float32),
                pltpu.VMEM((n_dev, 8, LANES), jnp.float32),
                pltpu.SMEM((rows,), jnp.float32),
                pltpu.SMEM((rows,), jnp.int32),
                pltpu.SemaphoreType.REGULAR,
                pltpu.SemaphoreType.DMA((3,)),
                pltpu.SemaphoreType.DMA((RING,)),
                pltpu.SemaphoreType.DMA((len(CHUNKS),)),
                pltpu.SemaphoreType.DMA((PUSHES,)),
                pltpu.SemaphoreType.DMA((PUSHES,)),
                pltpu.SemaphoreType.DMA((PUSHES,)),
                pltpu.SemaphoreType.DMA((PUSHES,)),
                pltpu.SemaphoreType.DMA((n_dev - 1,)),
                pltpu.SemaphoreType.DMA((n_dev - 1,)),
            ],
            compiler_params=pltpu.CompilerParams(
                collective_id=0, has_side_effects=True, vmem_limit_bytes=48 * 1024 * 1024
            ),
        )(*[pltpu.with_memory_space_constraint(x, pltpu.HBM) for x in (inv_temp, target, hidden, w_head)])
        return pl.pallas_call(
            finish_kernel,
            out_shape=(
                jax.ShapeDtypeStruct((rows, width), jnp.float32),
                jax.ShapeDtypeStruct((rows,), jnp.float32),
            ),
            in_specs=[vmem, vmem],
            out_specs=(hbm, hbm),
            scratch_shapes=[
                pltpu.VMEM((rows, width), jnp.float32),
                pltpu.VMEM((rows,), jnp.float32),
                pltpu.SemaphoreType.DMA((OUT_CHUNKS + 1,)),
            ],
            compiler_params=pltpu.CompilerParams(vmem_limit_bytes=8 * 1024 * 1024),
        )(mass, fin)

    vocab_axes = ("vblk", "vocab")
    return jax.shard_map(
        local_step,
        mesh=mesh,
        in_specs=(P("dp", None), P(None, vocab_axes), P("dp"), P("dp")),
        out_specs=(P("dp", vocab_axes), P("dp")),
        check_vma=False,
    )
```

```python
import functools

import jax
import jax.numpy as jnp
from jax import lax
from jax.experimental import pallas as pl
from jax.experimental.pallas import tpu as pltpu
from jax.sharding import PartitionSpec as P

MESH = pl.DeviceIdType.MESH
LANES = 128
GROUP = 256
TILE = 1024
LAST = 1280
CHUNKS = (2048, 1024)
RING = 4
PUSH = 512
PUSHES = 10
SLOTS = 4
OUT_CHUNKS = 5


def split_sums(e, tri):
    hi = e.astype(jnp.bfloat16)
    rest = e - hi.astype(jnp.float32)
    mid = rest.astype(jnp.bfloat16)
    low = (rest - mid.astype(jnp.float32)).astype(jnp.bfloat16)
    sums = jnp.dot(jnp.concatenate([hi, mid, low], axis=0), tri[...], preferred_element_type=jnp.float32)
    n = e.shape[0]
    return sums[:n] + (sums[n:2 * n] + sums[2 * n:])


def stream_kernel(
    vblk_size, vocab_size, tau_hbm, tgt_hbm, h_hbm, w_hbm, c_ref, fin_ref,
    h_buf, w_buf, last_buf, push_buf, z_out, z_in, z_late, z_last, tri, near_max, far_max, far, guest, pack, comm, tau_sm, tgt_sm,
    ready, in_sem, w_sem, last_sem, push_send, push_recv, z_send, z_recv, send_sem, recv_sem,
):
    n_dev = vblk_size * vocab_size
    rows, depth = h_buf.shape
    width = w_hbm.shape[1]
    pushed = PUSH * PUSHES
    n_full = (width - pushed - LAST) // TILE
    last_col = width - LAST
    parts = [pl.ds(sum(CHUNKS[:k]), size) for k, size in enumerate(CHUNKS)]
    vblk, vocab = lax.axis_index("vblk"), lax.axis_index("vocab")
    me = vblk * vocab_size + vocab
    chip, core = lax.div(vocab, 2), lax.rem(vocab, 2)
    sibling = {"vblk": vblk, "vocab": chip * 2 + (1 - core)}

    def peer_id(d):
        peer = lax.rem(me + d, n_dev)
        return {"vblk": lax.div(peer, vocab_size), "vocab": lax.rem(peer, vocab_size)}

    def near_col(t):
        return pl.multiple_of(pushed + t * TILE, LANES)

    def far_col(p):
        return pl.multiple_of(p * PUSH, LANES)

    def w_copy(t, slot):
        return pltpu.make_async_copy(w_hbm.at[:, pl.ds(near_col(t), TILE)], w_buf.at[slot], w_sem.at[slot])

    def last_copy(k):
        return pltpu.make_async_copy(
            w_hbm.at[parts[k], pl.ds(last_col, LAST)], last_buf.at[parts[k]], last_sem.at[k]
        )

    def push_copy(p):
        return pltpu.make_async_remote_copy(
            src_ref=w_hbm.at[:, pl.ds(far_col(p), PUSH)], dst_ref=push_buf.at[p % SLOTS],
            send_sem=push_send.at[p], recv_sem=push_recv.at[p], device_id=sibling, device_id_type=MESH,
        )

    def z_copy(p):
        return pltpu.make_async_remote_copy(
            src_ref=z_out.at[p], dst_ref=z_in.at[p],
            send_sem=z_send.at[p], recv_sem=z_recv.at[p], device_id=sibling, device_id_type=MESH,
        )

    barrier = pltpu.get_barrier_semaphore()

    @pl.when(core == 0)
    def _():
        pl.semaphore_signal(barrier, inc=1, device_id=sibling, device_id_type=MESH)

    small = [
        pltpu.make_async_copy(h_hbm, h_buf, in_sem.at[0]),
        pltpu.make_async_copy(tau_hbm, tau_sm, in_sem.at[1]),
        pltpu.make_async_copy(tgt_hbm, tgt_sm, in_sem.at[2]),
    ]
    for copy in small:
        copy.start()
    for t in range(RING - 1):
        w_copy(t, t).start()

    @pl.when(core == 1)
    def _():
        pl.semaphore_wait(barrier, 1)
        pl.semaphore_signal(ready, inc=1, device_id=sibling, device_id_type=MESH)

    @pl.when(core == 0)
    def _():
        pl.semaphore_wait(ready, 1)
        for d in range(2, n_dev, 2):
            pl.semaphore_signal(barrier, inc=1, device_id=peer_id(d), device_id_type=MESH)

    for p in range(2):
        push_copy(p).start()

    below = lax.broadcasted_iota(jnp.int32, tri.shape, 0)
    across = lax.broadcasted_iota(jnp.int32, tri.shape, 1)
    tri[...] = jnp.where((across >= GROUP) | (below <= across), 1.0, 0.0).astype(tri.dtype)

    for copy in small:
        copy.wait()
    row_id = lax.broadcasted_iota(jnp.int32, (rows, LANES), 0)
    lane_id = lax.broadcasted_iota(jnp.int32, (rows, LANES), 1)
    tau = jnp.zeros((rows, LANES), jnp.float32)
    tgt = jnp.zeros((rows, LANES), jnp.int32)
    for b in range(rows):
        tau = jnp.where(row_id == b, tau_sm[b], tau)
        tgt = jnp.where(row_id == b, tgt_sm[b], tgt)
    reach = tgt - me * width - lane_id
    host = vblk * vocab_size + chip * 2 + (1 - core)
    guest_reach = tgt - host * width - lane_id

    def blocks_of(x):
        return [x[:, j * LANES:(j + 1) * LANES] for j in range(x.shape[1] // LANES)]

    def softmax_step(col, z, top, total, pick, reach=reach):
        z = [zj * tau for zj in blocks_of(z)]
        peak = functools.reduce(jnp.maximum, z)
        new_top = jnp.maximum(top, jnp.max(peak, axis=1, keepdims=True))
        alpha = jnp.exp(top - new_top)
        e = [jnp.exp(zj - new_top) for zj in z]
        total = total * alpha + functools.reduce(jnp.add, e)
        hit = reach - col
        pick = pick * alpha + functools.reduce(
            jnp.add, [jnp.where(hit >= j * LANES, ej, 0.0) for j, ej in enumerate(e)]
        )
        return e, alpha, new_top, total, pick

    def prefix_step(col, e, base):
        groups = len(e) * LANES // GROUP
        stacked = jnp.concatenate([jnp.concatenate(e[2 * g:2 * g + 2], axis=1) for g in range(groups)], axis=0)
        sums = split_sums(stacked, tri)
        for g in range(groups):
            part_sums = sums[g * rows:(g + 1) * rows]
            for half in range(2):
                c_ref[:, pl.ds(col + (2 * g + half) * LANES, LANES)] = (
                    part_sums[:, half * LANES:(half + 1) * LANES] + base
                )
            base = base + part_sums[:, GROUP:]
        return base

    lowest, zero = jnp.full((rows, LANES), -jnp.inf, jnp.float32), jnp.zeros((rows, LANES), jnp.float32)
    far[0], far[1] = lowest, zero
    guest[0], guest[1], guest[2] = lowest, zero, zero

    def far_step(p):
        z_copy(p).wait_recv()
        e, alpha, top, _, _ = softmax_step(far_col(p), z_in[p], far[0], zero, zero)
        far[1] = prefix_step(far_col(p), e, far[1] * alpha)
        far[0] = top
        far_max[p] = top

    def near_step(t, z, state):
        top, base, total, pick = state
        e, alpha, top, total, pick = softmax_step(near_col(t), z, top, total, pick)
        base = prefix_step(near_col(t), e, base * alpha)
        near_max[t] = top
        return top, base, total, pick

    def near_dot(t):
        slot, ahead = lax.rem(t, RING), t + RING - 1
        w_copy(0, slot).wait()

        @pl.when(ahead < n_full)
        def _():
            w_copy(ahead, lax.rem(ahead, RING)).start()

        @pl.when(ahead == n_full)
        def _():
            for k in range(len(CHUNKS)):
                last_copy(k).start()

        return jnp.dot(h_buf[...], w_buf[slot], preferred_element_type=jnp.float32)

    def push_dot(p):
        push_copy(p).wait_recv()
        z = jnp.dot(h_buf[...], push_buf[lax.rem(p, SLOTS)], preferred_element_type=jnp.float32)
        z_out[p] = z
        _, _, guest[0], guest[1], guest[2] = softmax_step(far_col(p), z, guest[0], guest[1], guest[2], guest_reach)

    def answer(p):
        z_copy(p).start()

        @pl.when(p + 2 < PUSHES)
        def _():
            push_copy(p + 2).start()

    def round_step(u, state, first=False):
        t, p = 5 * u, 2 * u
        z = near_dot(t)
        if not first:
            state = near_step(t - 1, z_late[...], state)
            far_step(p - 2)
        z_next = near_dot(t + 1)
        state = near_step(t, z, state)
        z = near_dot(t + 2)
        state = near_step(t + 1, z_next, state)
        push_dot(p)
        z_next = near_dot(t + 3)
        state = near_step(t + 2, z, state)
        answer(p)
        if not first:
            far_step(p - 1)
        z = near_dot(t + 4)
        z_late[...] = z
        push_dot(p + 1)
        state = near_step(t + 3, z_next, state)
        answer(p + 1)
        return state

    state = (lowest, zero, zero, zero)
    state = round_step(jnp.int32(0), state, first=True)
    state = lax.fori_loop(1, n_full // 5, round_step, state)

    @pl.when(core == 0)
    def _():
        pl.semaphore_wait(barrier, n_dev // 2 - 1)
        pl.semaphore_signal(ready, inc=1, device_id=sibling, device_id_type=MESH)

    def last_dot(k):
        last_copy(k).wait()
        return jnp.dot(h_buf[:, parts[k]], last_buf[parts[k], :], preferred_element_type=jnp.float32)

    z_last[...] = last_dot(0)
    top, base, total, pick = near_step(n_full - 1, z_late[...], state)
    z = z_last[...]
    for k in range(1, len(CHUNKS)):
        z = z + last_dot(k)
    e, alpha, near_top, total, pick = softmax_step(last_col, z, top, total, pick)

    diag = row_id == lane_id
    to_lanes = lambda x: jnp.sum(jnp.where(diag, x, 0.0), axis=0, keepdims=True)
    row_sum = lambda x: jnp.broadcast_to(jnp.sum(x, axis=1, keepdims=True), x.shape)
    sub = lax.broadcasted_iota(jnp.int32, (8, LANES), 0)
    packet = jnp.zeros((8, LANES), jnp.float32)
    stats = (near_top, row_sum(total), row_sum(pick), guest[0], row_sum(guest[1]), row_sum(guest[2]))
    for i, stat in enumerate(stats):
        packet = jnp.where(sub == i, to_lanes(stat), packet)
    pack[...] = packet
    comm[me] = packet

    @pl.when(core == 1)
    def _():
        pl.semaphore_wait(ready, 1)

    copies = [
        pltpu.make_async_remote_copy(
            src_ref=pack, dst_ref=comm.at[me], send_sem=send_sem.at[d - 1], recv_sem=recv_sem.at[d - 1],
            device_id=peer_id(d), device_id_type=MESH,
        )
        for d in range(1, n_dev)
    ]
    for copy in copies:
        copy.start()

    far_step(PUSHES - 2)
    far_step(PUSHES - 1)
    top = jnp.maximum(near_top, far[0])
    near_scale, far_scale = jnp.exp(near_top - top), jnp.exp(far[0] - top)
    prefix_step(last_col, e, base * alpha)
    far_sum = far[1] * far_scale

    def rescale_near(t, carry):
        factor = jnp.exp(near_max[t] - top)
        for j in range(TILE // LANES):
            cols = pl.ds(near_col(t) + j * LANES, LANES)
            c_ref[:, cols] = c_ref[:, cols] * factor + far_sum
        return carry

    def rescale_far(p, carry):
        factor = jnp.exp(far_max[p] - top)
        for j in range(PUSH // LANES):
            cols = pl.ds(far_col(p) + j * LANES, LANES)
            c_ref[:, cols] = c_ref[:, cols] * factor
        return carry

    lax.fori_loop(0, n_full, rescale_near, 0)
    for j in range(LAST // LANES):
        cols = pl.ds(last_col + j * LANES, LANES)
        c_ref[:, cols] = c_ref[:, cols] * near_scale + far_sum
    lax.fori_loop(0, PUSHES, rescale_far, 0)
    for p in range(PUSHES):
        push_copy(p).wait_send()
        z_copy(p).wait_send()

    for copy in copies:
        copy.wait()
    dev = lax.broadcasted_iota(jnp.int32, (n_dev, LANES), 0)
    hosts = dev + 1 - 2 * lax.rem(dev, 2)
    tops, guest_tops = comm[:, 0, :], comm[:, 3, :]
    top_all = jnp.max(jnp.maximum(tops, guest_tops), axis=0, keepdims=True)
    scale, guest_scale = jnp.exp(tops - top_all), jnp.exp(guest_tops - top_all)
    mass, guest_mass = comm[:, 1, :] * scale, comm[:, 4, :] * guest_scale
    all_mass = jnp.sum(mass + guest_mass, axis=0, keepdims=True)
    lower = jnp.sum(jnp.where(dev < me, mass, 0.0) + jnp.where(hosts < me, guest_mass, 0.0), axis=0, keepdims=True)
    picked = jnp.sum(comm[:, 2, :] * scale + comm[:, 5, :] * guest_scale, axis=0, keepdims=True)
    mult = jnp.exp(to_lanes(top) - top_all) / all_mass
    fin_ref[...] = jnp.where(
        sub == 0, mult, jnp.where(sub == 1, lower / all_mass, jnp.where(sub == 2, picked / all_mass, 0.0))
    )


def finish_kernel(c_ref, fin_ref, cdf_hbm, picked_hbm, out_buf, picked_buf, out_sem):
    rows, width = c_ref.shape
    step = width // OUT_CHUNKS
    row_id = lax.broadcasted_iota(jnp.int32, (rows, LANES), 0)
    lane_id = lax.broadcasted_iota(jnp.int32, (rows, LANES), 1)
    fin = fin_ref[...]
    to_rows = lambda x: jnp.broadcast_to(
        jnp.sum(jnp.where(row_id == lane_id, x, 0.0), axis=1, keepdims=True), (rows, LANES)
    )
    mult, offset = to_rows(fin[0:1]), to_rows(fin[1:2])
    picked_buf[...] = fin[2, :rows]
    copies = [pltpu.make_async_copy(picked_buf, picked_hbm, out_sem.at[OUT_CHUNKS])]
    copies[0].start()
    for i in range(OUT_CHUNKS):
        for j in range(step // LANES):
            cols = pl.ds(i * step + j * LANES, LANES)
            out_buf[:, cols] = c_ref[:, cols] * mult + offset
        cols = pl.ds(i * step, step)
        copies.append(pltpu.make_async_copy(out_buf.at[:, cols], cdf_hbm.at[:, cols], out_sem.at[i]))
        copies[-1].start()
    for copy in copies:
        copy.wait()


def solution(mesh):
    vblk_size, vocab_size = mesh.shape["vblk"], mesh.shape["vocab"]
    n_dev = vblk_size * vocab_size

    def local_step(hidden, w_head, inv_temp, target):
        rows, depth = hidden.shape
        width = w_head.shape[1]
        hbm = pl.BlockSpec(memory_space=pltpu.HBM)
        vmem = pl.BlockSpec(memory_space=pltpu.VMEM)
        mass, fin = pl.pallas_call(
            functools.partial(stream_kernel, vblk_size, vocab_size),
            out_shape=(
                jax.ShapeDtypeStruct((rows, width), jnp.float32),
                jax.ShapeDtypeStruct((8, LANES), jnp.float32),
            ),
            in_specs=[hbm] * 4,
            out_specs=(vmem, vmem),
            scratch_shapes=[
                pltpu.VMEM((rows, depth), jnp.bfloat16),
                pltpu.VMEM((RING, depth, TILE), jnp.bfloat16),
                pltpu.VMEM((depth, LAST), jnp.bfloat16),
                pltpu.VMEM((SLOTS, depth, PUSH), jnp.bfloat16),
                pltpu.VMEM((PUSHES, rows, PUSH), jnp.float32),
                pltpu.VMEM((PUSHES, rows, PUSH), jnp.float32),
                pltpu.VMEM((rows, TILE), jnp.float32),
                pltpu.VMEM((rows, LAST), jnp.float32),
                pltpu.VMEM((GROUP, GROUP + LANES), jnp.bfloat16),
                pltpu.VMEM(((width - PUSH * PUSHES - LAST) // TILE, rows, LANES), jnp.float32),
                pltpu.VMEM((PUSHES, rows, LANES), jnp.float32),
                pltpu.VMEM((2, rows, LANES), jnp.float32),
                pltpu.VMEM((3, rows, LANES), jnp.float32),
                pltpu.VMEM((8, LANES), jnp.float32),
                pltpu.VMEM((n_dev, 8, LANES), jnp.float32),
                pltpu.SMEM((rows,), jnp.float32),
                pltpu.SMEM((rows,), jnp.int32),
                pltpu.SemaphoreType.REGULAR,
                pltpu.SemaphoreType.DMA((3,)),
                pltpu.SemaphoreType.DMA((RING,)),
                pltpu.SemaphoreType.DMA((len(CHUNKS),)),
                pltpu.SemaphoreType.DMA((PUSHES,)),
                pltpu.SemaphoreType.DMA((PUSHES,)),
                pltpu.SemaphoreType.DMA((PUSHES,)),
                pltpu.SemaphoreType.DMA((PUSHES,)),
                pltpu.SemaphoreType.DMA((n_dev - 1,)),
                pltpu.SemaphoreType.DMA((n_dev - 1,)),
            ],
            compiler_params=pltpu.CompilerParams(
                collective_id=0, has_side_effects=True, vmem_limit_bytes=48 * 1024 * 1024
            ),
        )(*[pltpu.with_memory_space_constraint(x, pltpu.HBM) for x in (inv_temp, target, hidden, w_head)])
        return pl.pallas_call(
            finish_kernel,
            out_shape=(
                jax.ShapeDtypeStruct((rows, width), jnp.float32),
                jax.ShapeDtypeStruct((rows,), jnp.float32),
            ),
            in_specs=[vmem, vmem],
            out_specs=(hbm, hbm),
            scratch_shapes=[
                pltpu.VMEM((rows, width), jnp.float32),
                pltpu.VMEM((rows,), jnp.float32),
                pltpu.SemaphoreType.DMA((OUT_CHUNKS + 1,)),
            ],
            compiler_params=pltpu.CompilerParams(vmem_limit_bytes=8 * 1024 * 1024),
        )(mass, fin)

    vocab_axes = ("vblk", "vocab")
    return jax.shard_map(
        local_step,
        mesh=mesh,
        in_specs=(P("dp", None), P(None, vocab_axes), P("dp"), P("dp")),
        out_specs=(P("dp", vocab_axes), P("dp")),
        check_vma=False,
    )
```
